128 devices in a mesh: pipe: 4 (over y_hi, core), exp: 16 (over x, z), pair: 2 (over y_lo).
Axes of the slice: x: 4, y: 4 (y_hi: 2, y_lo: 2; y = y_hi * 2 + y_lo), z: 4, core: 2. Of those that a mesh axis runs over, the one named last changes fastest.
Arguments:
- hidden_in: bfloat16 [4, 1024, 2048], P(None, ('exp', 'pair')), may hold values from -6 to 6
- routes: int32 [4, 4, 1024, 8], P('pipe', None, ('exp', 'pair')), may hold values from 0 to 63, all different within a row; in each aligned block of 32 rows (0 to 31, 32 to 63, ..., all dimensions but the last counted through in order) at most 6 rows name the same one
- gate_probs: float32 [4, 4, 1024, 8], P('pipe', None, ('exp', 'pair')), may hold values from 0.02 to 1
- norm_gain: float32 [4, 2048], P('pipe'), may hold values from 0.1 to 1.9
- w_gate: bfloat16 [4, 64, 2048, 768], P('pipe', ('exp', 'pair')), may hold values from -0.125 to 0.125
- w_up: bfloat16 [4, 64, 2048, 768], P('pipe', ('exp', 'pair')), may hold values from -0.125 to 0.125
- w_down: bfloat16 [4, 64, 768, 2048], P('pipe', ('exp', 'pair')), may hold values from -0.21875 to 0.21875
Outputs:
- layer_outputs: bfloat16 [4, 4, 1024, 2048], P('pipe', None, ('exp', 'pair'))
The draws below stay inside these ranges and needn't reach their ends.
Inputs may be any that keep to these rules, and one draw needn't show every extreme that they name: `routes`: within each layer and micro-batch, the 32 tokens of one device (aligned blocks) name no expert more than 6 times in all, and each token names 8 different experts.
All inputs are finite; a program needn't handle non-finite values.
Results may differ from the reference program's by a relative error of at most 0.01.
Values may be sent and summed in bfloat16 or wider, within the bound.
A program may use at most 64 MiB of HBM per device.

```python
import math
import jax
import jax.numpy as jnp
import numpy as np
from jax import lax

D = 2048
FF = 768
TOPK = 8
MB = 4
TOK_DEV = 32
EXPERTS = 64
LAYERS = 4
TOKENS = 1024
CAP = 6


def block_scale(rng, shape, shards, least, largest):
    def one(position, parts):
        steps = jax.random.uniform(jax.random.fold_in(jax.random.fold_in(rng, 6), position), (parts,), jnp.float32, least / len(shards), largest / len(shards))
        return jnp.repeat(jnp.exp(steps), shape[position] // parts).reshape((-1,) + (1,) * (len(shape) - position - 1))

    loudness = one(*shards[0])
    for cut in shards[1:]:
        loudness = loudness * one(*cut)
    return loudness


def routed_block(rng, own, number, rows, number_of, top, bound, skew):
    order = jax.random.permutation(rng, number_of)
    packed, common = shares(number_of, rows * top, bound, skew, True), shares(number_of, rows * top, bound, skew, False)
    places = jnp.arange(number_of)

    def named(sizes, rotation):
        used = int((sizes > 0).sum())
        fixed = max(1, used // 4)
        shifted = fixed + (places - fixed + rotation * (used - fixed)) % max(1, number_of - fixed)
        return jnp.zeros((number_of,), jnp.int32).at[order[jnp.where(places < fixed, places, shifted)]].set(jnp.asarray(sizes, jnp.int32))

    sizes = jnp.where(number % 4 == 0, named(packed, number // 4), named(common, number - number // 4 - 1))
    mixed = jax.random.permutation(jax.random.fold_in(own, 3), number_of)
    donor, taker = mixed[0:number_of // 2 * 2:2], mixed[1:number_of // 2 * 2:2]
    margin = jnp.minimum(sizes[donor] - 1, bound - sizes[taker]) // 2
    margin = jnp.where((donor == order[0]) | (taker == order[0]) | (sizes[taker] == 0), 0, jnp.maximum(margin, 0))
    shifted = jax.random.randint(jax.random.fold_in(own, 4), (number_of // 2,), 0, 1 << 20) % (margin + 1)
    sizes = sizes.at[donor].add(-shifted).at[taker].add(shifted)
    labels = jnp.searchsorted(jnp.cumsum(sizes), jnp.arange(rows * top), side="right").astype(jnp.int32)
    grid = labels.reshape(top, rows).T
    grid = grid[jax.random.permutation(jax.random.fold_in(own, 1), rows)]
    rotation = jax.random.randint(jax.random.fold_in(own, 2), (rows, 1), 0, top)
    return jnp.take_along_axis(grid, (jnp.arange(top)[None, :] + rotation) % top, axis=1)


def shares(number_of, total, most, skew, full):
    loads = [(1 << 20) // math.isqrt(grade ** skew) + 1 for grade in range(1, number_of + 1)]
    largest = most if full else min(most, max(-(-total // number_of), total * loads[0] // sum(loads)))
    least = 1 if total - largest >= number_of - 1 else 0
    counts, surplus = [largest] + [least] * (number_of - 1), total - largest - least * (number_of - 1)
    while surplus > 0:
        candidates = [i for i in range(1, number_of) if counts[i] < largest] or [i for i in range(1, number_of) if counts[i] < most]
        mass, remaining = sum([loads[i] for i in candidates]), surplus
        for i in candidates:
            addition = min(most - counts[i], max(1, remaining * loads[i] // mass), surplus)
            counts[i] = counts[i] + addition
            surplus = surplus - addition
    return np.array(counts)


def normal_values(own_key, dims, width, most, shards=(), held_as=jnp.bfloat16):
    drawn = jax.random.normal(own_key, dims, jnp.float32) * width
    if len(shards) > 0:
        drawn = block_scale(own_key, dims, shards, -0.22, 0.18) * drawn
    return jnp.clip(drawn, min=-most, max=most).astype(held_as)


def setup_inputs(seed: int = 0) -> dict:
    key_of = jax.random.split(jax.random.key(seed), 8)
    hidden_in = normal_values(key_of[0], (MB, TOKENS, D), 1.0, 6.0, ((1, 32),))
    routes_keys = jax.random.split(jax.random.fold_in(key_of[1], 1), LAYERS * MB * TOKENS // TOK_DEV)
    routes_turns = jax.random.permutation(jax.random.fold_in(key_of[1], 3), LAYERS * MB * TOKENS // TOK_DEV)
    routes = jax.vmap(lambda own, number: routed_block(jax.random.fold_in(key_of[1], 2), own, number, TOK_DEV, EXPERTS, TOPK, CAP, 2))(routes_keys, routes_turns).reshape((LAYERS, MB, TOKENS, TOPK))
    gate_probs = jnp.clip(jnp.exp(math.log(1.0) - 3.912023 * jax.random.uniform(key_of[2], (LAYERS, MB, TOKENS, TOPK), jnp.float32) ** block_scale(key_of[2], (LAYERS, MB, TOKENS, TOPK), ((0, 4), (2, 32)), -0.2, 0.2)), 0.02, 1.0)
    norm_gain = jnp.clip(1.0 + 0.18 * jax.random.normal(key_of[3], (LAYERS, D), jnp.float32), 0.1, 1.9)
    w_gate = normal_values(key_of[4], (LAYERS, EXPERTS, D, FF), D ** -0.5, 0.125, ((0, 4), (1, 32)))
    w_up = normal_values(key_of[5], (LAYERS, EXPERTS, D, FF), D ** -0.5, 0.125, ((0, 4), (1, 32)))
    w_down = normal_values(key_of[6], (LAYERS, EXPERTS, FF, D), FF ** -0.5, 0.21875, ((0, 4), (1, 32)))
    return {"hidden_in": hidden_in, "routes": routes, "gate_probs": gate_probs, "norm_gain": norm_gain, "w_gate": w_gate, "w_up": w_up, "w_down": w_down}


EPS = 1e-06

def slots_of(block_routes):
    expert_ids = jnp.arange(EXPERTS, dtype=jnp.int32)
    onehot = (block_routes[:, None] == expert_ids[None, :]).astype(jnp.int32)
    before = jnp.cumsum(onehot, axis=0) - onehot
    return lax.optimization_barrier(jnp.sum(before * onehot, axis=1)).astype(jnp.int32)

def moe_layer(state, chosen, probs, gain, wgate, wupper, wdown):
    floated = state.astype(jnp.float32)
    scale = lax.rsqrt(lax.optimization_barrier(jnp.mean(floated * floated, axis=-1, keepdims=True)) + EPS)
    normed = (floated * scale * gain.astype(jnp.float32)).astype(jnp.bfloat16)
    blocks = TOKENS // TOK_DEV
    flat_routes = chosen.reshape(blocks, TOK_DEV * TOPK).astype(jnp.int32)
    slots = jax.vmap(slots_of)(flat_routes)
    columns = (slots + CAP * jnp.arange(blocks, dtype=jnp.int32)[:, None]).reshape(-1)
    rows_ids = flat_routes.reshape(-1)
    buffer = jnp.zeros((EXPERTS, blocks * CAP, D), jnp.bfloat16)
    buffer = buffer.at[rows_ids, columns].set(jnp.repeat(normed, TOPK, axis=0))

    def one_expert(items):
        inputs, gate_w, up_w, down_w = items
        gate = jnp.dot(inputs, gate_w, preferred_element_type=jnp.float32)
        upward = jnp.dot(inputs, up_w, preferred_element_type=jnp.float32)
        hidden = (jax.nn.silu(gate) * upward).astype(jnp.bfloat16)
        return jnp.dot(hidden, down_w, preferred_element_type=jnp.float32).astype(jnp.bfloat16)
    produced = lax.map(one_expert, (buffer, wgate, wupper, wdown))
    picked = produced[rows_ids, columns].reshape(TOKENS, TOPK, D).astype(jnp.float32)
    probs32 = probs.astype(jnp.float32)
    weights = probs32 / lax.optimization_barrier(jnp.sum(probs32, axis=-1, keepdims=True))
    mixed = jnp.einsum('tk,tkd->td', weights, picked)
    return (floated + mixed).astype(jnp.bfloat16)

def reference(hidden_in, routes, gate_probs, norm_gain, w_gate, w_up, w_down):
    current = hidden_in
    outputs = []
    for layer in range(LAYERS):

        def per_batch(items):
            state, chosen, probs = items
            return moe_layer(state, chosen, probs, norm_gain[layer], w_gate[layer], w_up[layer], w_down[layer])
        current = lax.map(per_batch, (current, routes[layer], gate_probs[layer]))
        outputs.append(current)
    return jnp.stack(outputs, axis=0)
```

```python
import functools

import jax
import jax.numpy as jnp
from jax import lax
from jax.experimental import pallas as pl
from jax.experimental.pallas import tpu as pltpu
from jax.sharding import PartitionSpec as P

EPS = 1e-06
MESH = pl.DeviceIdType.MESH
SIDE = 4
BLOCKS = 2 * SIDE
CAP = 6
F32 = jnp.float32
BF16 = jnp.bfloat16


def kernel(
    sizes,
    hidden_ref, routes_ref, probs_ref, gain_ref, wg_hbm, wu_hbm, wd_hbm,
    out_ref,
    wg, wu, wd, hs, meta, grid, gmeta, outbox, inbox, back, part, parts, ysend, yrecv, acc,
    xin, hid, meta_t, pick, mix, expect, perm, perm_t,
    w_sem, h_r, h_s, y_r, ym_r, g_r, gm_r, g_s, gm_s, x_r, x_s, r_r, r_s, p_r, p_s, f_r, f_s,
):
    micro, tok, width, ff, local, stages = sizes
    half = width // 2
    rows = BLOCKS * CAP
    chunk = local * rows
    stage = lax.axis_index("pipe")
    e = lax.axis_index("exp")
    y = lax.axis_index("pair")
    x, z = e // SIDE, e % SIDE
    gather_at, send_at = (x, z), (z, x)

    def on_x(d):
        return {"exp": (x + d) % SIDE * SIDE + z}

    def on_z(d):
        return {"exp": x * SIDE + (z + d) % SIDE}

    gather_to, send_to = (on_x, on_z), (on_z, on_x)
    y_peer = {"pair": 1 - y}

    def push(src, dst, send, recv, to):
        pltpu.make_async_remote_copy(
            src_ref=src, dst_ref=dst, send_sem=send, recv_sem=recv, device_id=to, device_id_type=MESH
        ).start()

    def await_bytes(ref, sem):
        pltpu.make_async_copy(ref, ref, sem).wait()

    weight_copies = [
        pltpu.make_async_copy(src.at[0], dst, w_sem.at[i])
        for i, (src, dst) in enumerate(((wg_hbm, wg), (wu_hbm, wu), (wd_hbm, wd)))
    ]
    for copy in weight_copies:
        copy.start()

    barrier = pltpu.get_barrier_semaphore()
    greeted = [y_peer] + [f(d) for f in (on_x, on_z) for d in range(1, SIDE)]
    greeted += [{"pipe": (stage + d) % stages} for d in (1, stages - 1)]
    for to in greeted:
        pl.semaphore_signal(barrier, inc=1, device_id=to, device_id_type=MESH)

    every = micro * tok
    lane = lax.broadcasted_iota(jnp.int32, (every, 128), 1)
    expert = lane % 64
    probs = probs_ref[...]
    named = jnp.zeros((every, 128), F32)
    weight = jnp.zeros((every, 128), F32)
    for k in range(routes_ref.shape[1]):
        hit = routes_ref[:, k : k + 1] == expert
        named = jnp.where(hit, 1.0, named)
        weight = jnp.where(hit, probs[:, k : k + 1], weight)
    weight = weight / jnp.sum(probs, axis=-1, keepdims=True)
    r0 = lax.broadcasted_iota(jnp.int32, (every, every), 0)
    r1 = lax.broadcasted_iota(jnp.int32, (every, every), 1)
    earlier = jnp.where((r1 < r0) & (r1 // tok == r0 // tok), 1.0, 0.0).astype(BF16)
    before = jnp.dot(earlier, named.astype(BF16), preferred_element_type=F32)
    both = jnp.where(lane < 64, named * (before + 1.0), weight).astype(BF16)
    for m in range(micro):
        meta[m] = both[m * tok : (m + 1) * tok]

    q0 = lax.broadcasted_iota(jnp.int32, (rows, BLOCKS * tok), 0)
    q1 = lax.broadcasted_iota(jnp.int32, (rows, BLOCKS * tok), 1)
    expect[...] = jnp.where(q0 // CAP == q1 // tok, q0 % CAP + 1, -1).astype(F32)
    total = SIDE * rows
    piece = rows // SIDE
    s0 = lax.broadcasted_iota(jnp.int32, (total, total), 0)
    s1 = lax.broadcasted_iota(jnp.int32, (total, total), 1)
    perm[...] = jnp.where(
        s1 == s0 % rows // piece * rows + s0 // rows * piece + s0 % piece, 1.0, 0.0
    ).astype(BF16)

    pl.semaphore_wait(barrier, len(greeted))

    def normalize(m):
        @pl.when(stage == 0)
        def _():
            hs[m] = hidden_ref[m]

        @pl.when(stage > 0)
        def _():
            await_bytes(hs.at[m], h_r.at[m])

        floated = hs[m].astype(F32)
        scale = lax.rsqrt(jnp.mean(floated * floated, axis=-1, keepdims=True) + EPS)
        normed = (floated * scale * gain_ref[...]).astype(BF16)
        for h in range(2):
            mine = gather_at[h] * 2 + y
            grid[h, m, mine] = normed[:, h * half : (h + 1) * half]
            gmeta[h, m, mine] = meta[m]
        for h in range(2):
            mine = gather_at[h] * 2 + y
            block, tag = grid.at[h, m, mine], gmeta.at[h, m, mine]
            push(tag, tag, gm_s.at[h, m], ym_r.at[h, m], y_peer)
            push(block, block, g_s.at[h, m], y_r.at[h, m], y_peer)
        for h in range(2):
            mine = gather_at[h] * 2 + y
            block, tag = grid.at[h, m, mine], gmeta.at[h, m, mine]
            for d in (2, 1, 3):
                push(tag, tag, gm_s.at[h, m], gm_r.at[h, m], gather_to[h](d))
                push(block, block, g_s.at[h, m], g_r.at[h, m], gather_to[h](d))

    def forward(m):
        for h in range(2):
            other = gather_at[h] * 2 + 1 - y
            block, tag = grid.at[h, m, other], gmeta.at[h, m, other]
            await_bytes(tag, ym_r.at[h, m])
            await_bytes(block, y_r.at[h, m])
            for d in (2, 1, 3):
                push(tag, tag, gm_s.at[h, m], gm_r.at[h, m], gather_to[h](d))
                push(block, block, g_s.at[h, m], g_r.at[h, m], gather_to[h](d))

    def dispatch(m):
        for h in range(2):
            await_bytes(gmeta.at[h, m, 0 : BLOCKS - 2], gm_r.at[h, m])
            tags = gmeta[h, m].reshape(BLOCKS * tok, 128).astype(F32)
            meta_t[h] = tags.T
            for a in range(SIDE):
                owner = (x * SIDE + a) if h == 0 else (a * SIDE + z)
                for l in range(local):
                    at = (owner * 2 + y) * local + l
                    code = meta_t[h, pl.ds(at, 1), :]
                    to = slice((a * local + l) * rows, (a * local + l + 1) * rows)
                    pick[h, to] = jnp.where(code == expect[...], 1.0, 0.0).astype(BF16)
        for h in range(2):
            await_bytes(grid.at[h, m, 0 : BLOCKS - 2], g_r.at[h, m])
            for n in range(0, half, 512):
                chosen = jnp.dot(
                    pick[h],
                    grid[h, m, :, :, n : n + 512].reshape(BLOCKS * tok, 512),
                    preferred_element_type=F32,
                )
                outbox[h, m, :, :, :, n : n + 512] = chosen.astype(BF16).reshape(SIDE, local, rows, 512)
            own = send_at[h]
            for d in (2, 1, 3):
                push(
                    outbox.at[h, m, (own + d) % SIDE], inbox.at[h, m, own],
                    x_s.at[h, m], x_r.at[h, m], send_to[h](d),
                )
            inbox[h, m, own] = outbox[h, m, own]
        for h in range(2):
            for a in range(SIDE):
                owner = (x * SIDE + a) if h == 0 else (a * SIDE + z)
                for l in range(local):
                    at = (owner * 2 + y) * local + l
                    code = meta_t[h, pl.ds(at, 1), :]
                    share = meta_t[h, pl.ds(64 + at, 1), :]
                    to = slice((a * local + l) * rows, (a * local + l + 1) * rows)
                    mix[h, m % 2, to] = jnp.where(code == expect[...], share, 0.0)

    def experts(m):
        for h in range(2):
            await_bytes(inbox.at[h, m, 0 : SIDE - 1], x_r.at[h, m])
            await_bytes(outbox.at[h, m, 0 : SIDE - 1], x_s.at[h, m])
        for l in range(local):
            xin[l, :, 0:half] = inbox[0, m, :, l].reshape(total, half)
            for n in range(0, half, 512):
                turned = jnp.dot(
                    perm[...], inbox[1, m, :, l, :, n : n + 512].reshape(total, 512), preferred_element_type=F32
                )
                xin[l, :, half + n : half + n + 512] = turned.astype(BF16)
        for l in range(local):
            for n in range(0, ff, 256):
                gate = jnp.dot(xin[l], wg[l, :, n : n + 256], preferred_element_type=F32)
                upward = jnp.dot(xin[l], wu[l, :, n : n + 256], preferred_element_type=F32)
                hid[l, :, n : n + 256] = (jax.nn.silu(gate) * upward).astype(BF16)
        for h in range(2):
            for l in range(local):
                hidden = hid[l]
                if h == 1:
                    hidden = jnp.dot(perm[...], hidden, preferred_element_type=F32).astype(BF16)
                for n in range(0, half, 256):
                    made = jnp.dot(hidden, wd[l, :, h * half + n : h * half + n + 256], preferred_element_type=F32)
                    outbox[h, m, :, l, :, n : n + 256] = made.astype(BF16).reshape(SIDE, rows, 256)
            own = send_at[h]
            for d in (2, 1, 3):
                push(
                    outbox.at[h, m, (own + d) % SIDE], back.at[h, m, own],
                    r_s.at[h, m], r_r.at[h, m], send_to[h](d),
                )
            back[h, m, own] = outbox[h, m, own]

    def combine(m):
        for h in range(2):
            await_bytes(back.at[h, m, 0 : SIDE - 1], r_r.at[h, m])
            shares = mix[h, m % 2].T.astype(BF16)
            for n in range(0, half, 512):
                summed = jnp.dot(
                    shares,
                    back[h, m, :, :, :, n : n + 512].reshape(SIDE * chunk, 512),
                    preferred_element_type=F32,
                )
                part[h, m, :, :, n : n + 512] = summed.astype(BF16).reshape(SIDE, 2 * tok, 512)
            own = gather_at[h]
            for d in (2, 1, 3):
                push(
                    part.at[h, m, (own + d) % SIDE], parts.at[h, m, own],
                    p_s.at[h, m], p_r.at[h, m], gather_to[h](d),
                )

    def reduce(m):
        for h in range(2):
            await_bytes(parts.at[h, m, 0 : SIDE - 1], p_r.at[h, m])
            own = gather_at[h]

            def total_of(side):
                at = pl.ds(pl.multiple_of(side * tok, tok), tok)
                value = part[h, m, own, at].astype(F32)
                for d in range(1, SIDE):
                    value = value + parts[h, m, (own + d) % SIDE, at].astype(F32)
                return value

            ysend[h, m] = total_of(1 - y).astype(BF16)
            push(ysend.at[h, m], yrecv.at[h, m], f_s.at[h, m], f_r.at[h, m], y_peer)
            acc[h] = total_of(y)

    def finish(m):
        for h in range(2):
            await_bytes(yrecv.at[h, m], f_r.at[h, m])
            at = slice(h * half, (h + 1) * half)
            out_ref[m, :, at] = (hs[m, :, at].astype(F32) + (acc[h] + yrecv[h, m].astype(F32))).astype(BF16)

        @pl.when(stage < stages - 1)
        def _():
            push(out_ref.at[m], hs.at[m], h_s.at[m], h_r.at[m], {"pipe": stage + 1})

    def step(i, _):
        @pl.when(i == 1)
        def _():
            for copy in weight_copies:
                copy.wait()

        @pl.when(i > 0)
        def _():
            experts(i - 1)

        @pl.when(i < micro)
        def _():
            normalize(i)
            forward(i)

        @pl.when(i > 0)
        def _():
            combine(i - 1)

        @pl.when(i < micro)
        def _():
            dispatch(i)

        @pl.when(i > 0)
        def _():
            reduce(i - 1)
            finish(i - 1)

        return 0

    lax.fori_loop(0, micro + 1, step, 0)

    def drain(m, _):
        for h in range(2):
            await_bytes(grid.at[h, m, 0 : BLOCKS - 1], g_s.at[h, m])
            await_bytes(gmeta.at[h, m, 0 : BLOCKS - 1], gm_s.at[h, m])
            await_bytes(outbox.at[h, m, 0 : SIDE - 1], r_s.at[h, m])
            await_bytes(part.at[h, m, 0 : SIDE - 1], p_s.at[h, m])
            await_bytes(ysend.at[h, m], f_s.at[h, m])

        @pl.when(stage < stages - 1)
        def _():
            await_bytes(out_ref.at[m], h_s.at[m])

        return 0

    lax.fori_loop(0, micro, drain, 0)


def on_device(stages, hidden_in, routes, gate_probs, norm_gain, w_gate, w_up, w_down):
    micro, tok, width = hidden_in.shape
    top = routes.shape[3]
    local, ff = w_gate.shape[1], w_gate.shape[3]
    half = width // 2
    rows = BLOCKS * CAP
    sizes = (micro, tok, width, ff, local, stages)
    vmem = pl.BlockSpec(memory_space=pltpu.VMEM)
    hbm = pl.BlockSpec(memory_space=pl.ANY)
    pair = pltpu.SemaphoreType.DMA((2, micro))
    single = pltpu.SemaphoreType.DMA((micro,))
    out = pl.pallas_call(
        functools.partial(kernel, sizes),
        out_shape=jax.ShapeDtypeStruct((micro, tok, width), BF16),
        in_specs=[vmem, vmem, vmem, vmem, hbm, hbm, hbm],
        out_specs=vmem,
        scratch_shapes=[
            pltpu.VMEM((local, width, ff), BF16),
            pltpu.VMEM((local, width, ff), BF16),
            pltpu.VMEM((local, ff, width), BF16),
            pltpu.VMEM((micro, tok, width), BF16),
            pltpu.VMEM((micro, tok, 128), BF16),
            pltpu.VMEM((2, micro, BLOCKS, tok, half), BF16),
            pltpu.VMEM((2, micro, BLOCKS, tok, 128), BF16),
            pltpu.VMEM((2, micro, SIDE, local, rows, half), BF16),
            pltpu.VMEM((2, micro, SIDE, local, rows, half), BF16),
            pltpu.VMEM((2, micro, SIDE, local, rows, half), BF16),
            pltpu.VMEM((2, micro, SIDE, 2 * tok, half), BF16),
            pltpu.VMEM((2, micro, SIDE, 2 * tok, half), BF16),
            pltpu.VMEM((2, micro, tok, half), BF16),
            pltpu.VMEM((2, micro, tok, half), BF16),
            pltpu.VMEM((2, tok, half), F32),
            pltpu.VMEM((local, SIDE * rows, width), BF16),
            pltpu.VMEM((local, SIDE * rows, ff), BF16),
            pltpu.VMEM((2, 128, BLOCKS * tok), F32),
            pltpu.VMEM((2, SIDE * local * rows, BLOCKS * tok), BF16),
            pltpu.VMEM((2, 2, SIDE * local * rows, BLOCKS * tok), F32),
            pltpu.VMEM((rows, BLOCKS * tok), F32),
            pltpu.VMEM((SIDE * rows, SIDE * rows), BF16),
            pltpu.VMEM((8, 128), F32),
            pltpu.SemaphoreType.DMA((3,)),
            single, single, pair, pair, pair, pair, pair, pair, pair, pair, pair, pair, pair, pair, pair, pair,
        ],
        compiler_params=pltpu.CompilerParams(
            collective_id=0, has_side_effects=True, vmem_limit_bytes=67043328
        ),
        name="relay",
    )(
        hidden_in,
        routes.reshape(micro * tok, top),
        gate_probs.reshape(micro * tok, top),
        norm_gain,
        w_gate,
        w_up,
        w_down,
    )
    return out[None]


def solution(mesh):
    in_specs = (
        P(None, ("exp", "pair"), None),
        P("pipe", None, ("exp", "pair"), None),
        P("pipe", None, ("exp", "pair"), None),
        P("pipe", None),
        P("pipe", ("exp", "pair"), None, None),
        P("pipe", ("exp", "pair"), None, None),
        P("pipe", ("exp", "pair"), None, None),
    )
    out_specs = P("pipe", None, ("exp", "pair"), None)
    return jax.shard_map(
        functools.partial(on_device, mesh.shape["pipe"]),
        mesh=mesh,
        in_specs=in_specs,
        out_specs=out_specs,
        check_vma=False,
    )
```

```python
import functools

import jax
import jax.numpy as jnp
from jax import lax
from jax.experimental import pallas as pl
from jax.experimental.pallas import tpu as pltpu
from jax.sharding import PartitionSpec as P

EPS = 1e-06
MESH = pl.DeviceIdType.MESH
SIDE = 4
BLOCKS = 2 * SIDE
ORDER = (
    ("normalize", 0), ("prepare", 0), ("combine", 1), ("dispatch", 0), ("reduce", 1), ("finish", 1), ("experts", 0),
)
PIECES = 4
CAP = 6
F32 = jnp.float32
BF16 = jnp.bfloat16


def kernel(
    sizes,
    hidden_ref, routes_ref, probs_ref, gain_ref, wg_hbm, wu_hbm, wd_hbm,
    out_ref,
    wg, wu, wd, hs, grid, gmeta, outbox, inbox, back, part, parts, ysend, yrecv, acc,
    xin, sums, hid, turned, meta_t, pick, mix, shares, expect, perm,
    w_sem, ym_r, gm_r, gm_s, i_s, h_r, h_s, o_r, o_s,
    g_r, g_s, x_r, x_s, r_r, r_s, p_r, p_s, f_r, f_s,
):
    micro, tok, width, ff, local, stages = sizes
    half = width // 2
    span = half // PIECES
    order = [(c, h) for c in range(PIECES) for h in range(2)]
    rows = BLOCKS * CAP
    chunk = local * rows
    stage = lax.axis_index("pipe")
    e = lax.axis_index("exp")
    y = lax.axis_index("pair")
    x, z = e // SIDE, e % SIDE
    gather_at, send_at = (x, z), (z, x)

    def on_x(d):
        return {"exp": (x + d) % SIDE * SIDE + z}

    def on_z(d):
        return {"exp": x * SIDE + (z + d) % SIDE}

    gather_to, send_to = (on_x, on_z), (on_z, on_x)
    y_peer = {"pair": 1 - y}

    def push(src, dst, send, recv, to):
        pltpu.make_async_remote_copy(
            src_ref=src, dst_ref=dst, send_sem=send, recv_sem=recv, device_id=to, device_id_type=MESH
        ).start()

    def await_bytes(ref, sem):
        with jax.named_scope("wait"):
            pltpu.make_async_copy(ref, ref, sem).wait()

    weight_copies = [
        pltpu.make_async_copy(src.at[0], dst, w_sem.at[i])
        for i, (src, dst) in enumerate(((wg_hbm, wg), (wu_hbm, wu), (wd_hbm, wd)))
    ]
    for copy in weight_copies:
        copy.start()

    barrier = pltpu.get_barrier_semaphore()
    greeted = [y_peer] + [f(d) for f in (on_x, on_z) for d in range(1, SIDE)]
    greeted += [{"pipe": (stage + d) % stages} for d in (1, stages - 1)]
    greeted += [{"pipe": (stage + d) % stages, "pair": 1 - y} for d in (1, stages - 1)]
    for to in greeted:
        pl.semaphore_signal(barrier, inc=1, device_id=to, device_id_type=MESH)

    lane = lax.broadcasted_iota(jnp.int32, (tok, 128), 1)
    expert = (lane % 64).astype(F32)
    r0 = lax.broadcasted_iota(jnp.int32, (tok, tok), 0)
    r1 = lax.broadcasted_iota(jnp.int32, (tok, tok), 1)
    earlier = jnp.where(r1 < r0, 1.0, 0.0)
    eye = jnp.where(r1 == r0, 1.0, 0.0)
    last = (((1,), (1,)), ((), ()))
    for m in range(micro):
        chosen = lax.dot_general(eye, routes_ref[m].astype(F32), last, preferred_element_type=F32, precision="highest")
        probs = lax.dot_general(eye, probs_ref[m], last, preferred_element_type=F32, precision="highest")
        named = jnp.zeros((tok, 128), F32)
        weight = jnp.zeros((tok, 128), F32)
        for k in range(routes_ref.shape[1]):
            hit = chosen[:, k : k + 1] == expert
            named = jnp.where(hit, 1.0, named)
            weight = jnp.where(hit, probs[:, k : k + 1], weight)
        weight = weight / jnp.sum(probs, axis=-1, keepdims=True)
        before = jnp.dot(earlier, named, preferred_element_type=F32)
        both = jnp.where(lane < 64, named * (before + 1.0), weight).astype(BF16)
        for h in range(2):
            gmeta[h, gather_at[h] * 2 + y, m] = both

    q0 = lax.broadcasted_iota(jnp.int32, (rows, BLOCKS * tok), 0)
    q1 = lax.broadcasted_iota(jnp.int32, (rows, BLOCKS * tok), 1)
    expect[...] = jnp.where(q0 // CAP == q1 // tok, q0 % CAP + 1, -1).astype(F32)
    total = SIDE * rows
    piece = rows // SIDE
    s0 = lax.broadcasted_iota(jnp.int32, (total, total), 0)
    s1 = lax.broadcasted_iota(jnp.int32, (total, total), 1)
    perm[...] = jnp.where(
        s1 == s0 % rows // piece * rows + s0 // rows * piece + s0 % piece, 1.0, 0.0
    ).astype(BF16)

    @pl.when(stage == 0)
    def _():
        for m in range(micro):
            hs[m, y] = hidden_ref[m]

    with jax.named_scope("greet"):
        pl.semaphore_wait(barrier, len(greeted))

    def offer(m):
        push(hidden_ref.at[m], hs.at[m, y], i_s.at[m], o_r.at[m], y_peer)

    @pl.when(stage == 0)
    def _():
        offer(0)

    for h in range(2):
        tag = gmeta.at[h, gather_at[h] * 2 + y]
        push(tag, tag, gm_s.at[h], ym_r.at[h], y_peer)
        for d in (2, 1, 3):
            push(tag, tag, gm_s.at[h], gm_r.at[h], gather_to[h](d))

    def exchange_tags():
        for h in range(2):
            tag = gmeta.at[h, gather_at[h] * 2 + 1 - y]
            await_bytes(tag, ym_r.at[h])
            for d in (2, 1, 3):
                push(tag, tag, gm_s.at[h], gm_r.at[h], gather_to[h](d))

        for h in range(2):
            await_bytes(gmeta.at[h, 0 : BLOCKS - 2], gm_r.at[h])

    @pl.when(stage > 0)
    def _():
        exchange_tags()

    def prepare(m):
        for h in range(2):
            tags = gmeta[h, :, m].reshape(BLOCKS * tok, 128).astype(F32)
            meta_t[h] = tags.T
            for a in range(SIDE):
                owner = (x * SIDE + a) if h == 0 else (a * SIDE + z)
                for l in range(local):
                    at = (owner * 2 + y) * local + l
                    hit = meta_t[h, pl.ds(at, 1), :] == expect[...]
                    share = meta_t[h, pl.ds(64 + at, 1), :]
                    to = slice((a * local + l) * rows, (a * local + l + 1) * rows)
                    pick[h, to] = jnp.where(hit, 1.0, 0.0).astype(BF16)
                    mix[h, to] = jnp.where(hit, share, 0.0)
            shares[m % 2, h] = mix[h].T.astype(BF16)

    def normalize(m):
        @pl.when(stage > 0)
        def _():
            await_bytes(hs.at[m, y], h_r.at[m])

        for turn in range(2):
            pair = y if turn == 0 else 1 - y
            if turn == 1:
                await_bytes(hs.at[m, pair], o_r.at[m])
            floated = hs[m, pair].astype(F32)
            scale = lax.rsqrt(jnp.mean(floated * floated, axis=-1, keepdims=True) + EPS)
            normed = (floated * scale * gain_ref[...]).astype(BF16)
            for c, h in order:
                at = h * half + c * span
                grid[h, c, m, gather_at[h] * 2 + pair] = normed[:, at : at + span]
            for c, h in order:
                block = grid.at[h, c, m, gather_at[h] * 2 + pair]
                for d in (2, 1, 3):
                    push(block, block, g_s.at[h, c, m], g_r.at[h, c, m], gather_to[h](d))

    def dispatch(m):
        for c, h in order:
            await_bytes(grid.at[h, c, m, 0 : BLOCKS - 2], g_r.at[h, c, m])
            chosen = jnp.dot(
                pick[h], grid[h, c, m].reshape(BLOCKS * tok, span), preferred_element_type=F32
            ).astype(BF16)
            outbox[h, c, m] = chosen.reshape(SIDE, local, rows, span)
            own = send_at[h]
            for d in (2, 1, 3):
                push(
                    outbox.at[h, c, m, (own + d) % SIDE], inbox.at[h, c, m, own],
                    x_s.at[h, c, m], x_r.at[h, c, m], send_to[h](d),
                )
            inbox[h, c, m, own] = outbox[h, c, m, own]

    def experts(m):
        for c in range(PIECES):
            for h in range(2):
                await_bytes(inbox.at[h, c, m, 0 : SIDE - 1], x_r.at[h, c, m])
                await_bytes(outbox.at[h, c, m, 0 : SIDE - 1], x_s.at[h, c, m])
            for l in range(local):
                xin[l] = jnp.dot(
                    perm[...], inbox[1, c, m, :, l].reshape(total, span), preferred_element_type=F32
                ).astype(BF16)
            low, high = slice(c * span, (c + 1) * span), slice(half + c * span, half + (c + 1) * span)
            for l in range(local):
                for n in range(0, ff, 256):
                    to = slice(n, n + 256)
                    gate, upward = [
                        jnp.dot(inbox[0, c, m, :, l].reshape(total, span), w[l, low, to], preferred_element_type=F32)
                        + jnp.dot(xin[l], w[l, high, to], preferred_element_type=F32)
                        for w in (wg, wu)
                    ]
                    if c > 0:
                        gate, upward = gate + sums[0, l, :, to], upward + sums[1, l, :, to]
                    if c < PIECES - 1:
                        sums[0, l, :, to], sums[1, l, :, to] = gate, upward
                    else:
                        hid[l, :, to] = (jax.nn.silu(gate) * upward).astype(BF16)
        for c, h in order:
            for l in range(local):
                if h == 1 and c == 0:
                    turned[l] = jnp.dot(perm[...], hid[l], preferred_element_type=F32).astype(BF16)
                for n in range(0, span, 256):
                    at = h * half + c * span + n
                    made = jnp.dot(
                        hid[l] if h == 0 else turned[l], wd[l, :, at : at + 256], preferred_element_type=F32
                    )
                    outbox[h, c, m, :, l, :, n : n + 256] = made.astype(BF16).reshape(SIDE, rows, 256)
            own = send_at[h]
            for d in (2, 1, 3):
                push(
                    outbox.at[h, c, m, (own + d) % SIDE], back.at[h, c, m, own],
                    r_s.at[h, c, m], r_r.at[h, c, m], send_to[h](d),
                )
            back[h, c, m, own] = outbox[h, c, m, own]

    def combine(m):
        for c, h in order:
            await_bytes(back.at[h, c, m, 0 : SIDE - 1], r_r.at[h, c, m])
            summed = jnp.dot(
                shares[m % 2, h], back[h, c, m].reshape(SIDE * chunk, span), preferred_element_type=F32
            )
            part[h, c, m] = summed.astype(BF16).reshape(SIDE, 2 * tok, span)
            own = gather_at[h]
            for d in (2, 1, 3):
                push(
                    part.at[h, c, m, (own + d) % SIDE], parts.at[h, c, m, own],
                    p_s.at[h, c, m], p_r.at[h, c, m], gather_to[h](d),
                )

    def reduce(m):
        for c, h in order:
            await_bytes(parts.at[h, c, m, 0 : SIDE - 1], p_r.at[h, c, m])
            own = gather_at[h]

            def total_of(side):
                at = pl.ds(pl.multiple_of(side * tok, tok), tok)
                value = part[h, c, m, own, at].astype(F32)
                for d in range(1, SIDE):
                    value = value + parts[h, c, m, (own + d) % SIDE, at].astype(F32)
                return value

            ysend[h, c, m] = total_of(1 - y).astype(BF16)
            push(ysend.at[h, c, m], yrecv.at[h, c, m], f_s.at[h, c, m], f_r.at[h, c, m], y_peer)
            acc[h, c] = total_of(y)

    def finish(m):
        for c, h in order:
            await_bytes(yrecv.at[h, c, m], f_r.at[h, c, m])
            at = slice(h * half + c * span, h * half + (c + 1) * span)
            out_ref[m, :, at] = (
                hs[m, y, :, at].astype(F32) + (acc[h, c] + yrecv[h, c, m].astype(F32))
            ).astype(BF16)

            @pl.when(stage < stages - 1)
            def _():
                done, there = out_ref.at[m, :, at], hs.at[m, y, :, at]
                push(done, there, o_s.at[m], o_r.at[m], {"pipe": stage + 1, "pair": 1 - y})
                push(done, there, h_s.at[m], h_r.at[m], {"pipe": stage + 1})

    tasks = {
        "prepare": prepare, "normalize": normalize, "dispatch": dispatch, "experts": experts,
        "combine": combine, "reduce": reduce, "finish": finish,
    }

    def step(i, _):
        for name, lag in ORDER:

            @pl.when((i >= lag) & (i < micro + lag))
            def _():
                with jax.named_scope(name):
                    if name == "experts":

                        @pl.when(i == lag)
                        def _():
                            for copy in weight_copies:
                                copy.wait()

                    if name == "prepare":

                        @pl.when((i == lag) & (stage == 0))
                        def _():
                            exchange_tags()
                            for m in range(1, micro):
                                offer(m)

                    tasks[name](i - lag)

        return 0

    lax.fori_loop(0, micro + max(lag for _, lag in ORDER), step, 0)

    for h in range(2):
        await_bytes(gmeta.at[h, 0 : BLOCKS - 1], gm_s.at[h])

    def drain(m, _):
        for c, h in order:
            await_bytes(grid.at[h, c, m, 0 : BLOCKS - 2], g_s.at[h, c, m])
            await_bytes(outbox.at[h, c, m, 0 : SIDE - 1], r_s.at[h, c, m])
            await_bytes(part.at[h, c, m, 0 : SIDE - 1], p_s.at[h, c, m])
            await_bytes(ysend.at[h, c, m], f_s.at[h, c, m])

        @pl.when(stage == 0)
        def _():
            await_bytes(hidden_ref.at[m], i_s.at[m])

        @pl.when(stage < stages - 1)
        def _():
            await_bytes(out_ref.at[m], h_s.at[m])
            await_bytes(out_ref.at[m], o_s.at[m])

        return 0

    lax.fori_loop(0, micro, drain, 0)


def on_device(stages, hidden_in, routes, gate_probs, norm_gain, w_gate, w_up, w_down):
    micro, tok, width = hidden_in.shape
    local, ff = w_gate.shape[1], w_gate.shape[3]
    span = width // 2 // PIECES
    rows = BLOCKS * CAP
    sizes = (micro, tok, width, ff, local, stages)
    vmem = pl.BlockSpec(memory_space=pltpu.VMEM)
    hbm = pl.BlockSpec(memory_space=pl.ANY)
    pair = pltpu.SemaphoreType.DMA((2, PIECES, micro))
    halves = pltpu.SemaphoreType.DMA((2,))
    single = pltpu.SemaphoreType.DMA((micro,))
    out = pl.pallas_call(
        functools.partial(kernel, sizes),
        out_shape=jax.ShapeDtypeStruct((micro, tok, width), BF16),
        in_specs=[vmem, vmem, vmem, vmem, hbm, hbm, hbm],
        out_specs=vmem,
        scratch_shapes=[
            pltpu.VMEM((local, width, ff), BF16),
            pltpu.VMEM((local, width, ff), BF16),
            pltpu.VMEM((local, ff, width), BF16),
            pltpu.VMEM((micro, 2, tok, width), BF16),
            pltpu.VMEM((2, PIECES, micro, BLOCKS, tok, span), BF16),
            pltpu.VMEM((2, BLOCKS, micro, tok, 128), BF16),
            pltpu.VMEM((2, PIECES, micro, SIDE, local, rows, span), BF16),
            pltpu.VMEM((2, PIECES, micro, SIDE, local, rows, span), BF16),
            pltpu.VMEM((2, PIECES, micro, SIDE, local, rows, span), BF16),
            pltpu.VMEM((2, PIECES, micro, SIDE, 2 * tok, span), BF16),
            pltpu.VMEM((2, PIECES, micro, SIDE, 2 * tok, span), BF16),
            pltpu.VMEM((2, PIECES, micro, tok, span), BF16),
            pltpu.VMEM((2, PIECES, micro, tok, span), BF16),
            pltpu.VMEM((2, PIECES, tok, span), F32),
            pltpu.VMEM((local, SIDE * rows, span), BF16),
            pltpu.VMEM((2, local, SIDE * rows, ff), F32),
            pltpu.VMEM((local, SIDE * rows, ff), BF16),
            pltpu.VMEM((local, SIDE * rows, ff), BF16),
            pltpu.VMEM((2, 128, BLOCKS * tok), F32),
            pltpu.VMEM((2, SIDE * local * rows, BLOCKS * tok), BF16),
            pltpu.VMEM((2, SIDE * local * rows, BLOCKS * tok), F32),
            pltpu.VMEM((2, 2, BLOCKS * tok, SIDE * local * rows), BF16),
            pltpu.VMEM((rows, BLOCKS * tok), F32),
            pltpu.VMEM((SIDE * rows, SIDE * rows), BF16),
            pltpu.SemaphoreType.DMA((3,)),
            halves, halves, halves, single, single, single, single, single,
            pair, pair, pair, pair, pair, pair, pair, pair, pair, pair,
        ],
        compiler_params=pltpu.CompilerParams(
            collective_id=0, has_side_effects=True, vmem_limit_bytes=67043328
        ),
        name="relay",
    )(
        hidden_in,
        jnp.swapaxes(routes[0], 1, 2),
        jnp.swapaxes(gate_probs[0], 1, 2),
        norm_gain,
        w_gate,
        w_up,
        w_down,
    )
    return out[None]


def solution(mesh):
    in_specs = (
        P(None, ("exp", "pair"), None),
        P("pipe", None, ("exp", "pair"), None),
        P("pipe", None, ("exp", "pair"), None),
        P("pipe", None),
        P("pipe", ("exp", "pair"), None, None),
        P("pipe", ("exp", "pair"), None, None),
        P("pipe", ("exp", "pair"), None, None),
    )
    out_specs = P("pipe", None, ("exp", "pair"), None)
    return jax.shard_map(
        functools.partial(on_device, mesh.shape["pipe"]),
        mesh=mesh,
        in_specs=in_specs,
        out_specs=out_specs,
        check_vma=False,
    )
```

```python
import functools

import jax
import jax.numpy as jnp
from jax import lax
from jax.experimental import pallas as pl
from jax.experimental.pallas import tpu as pltpu
from jax.sharding import PartitionSpec as P

EPS = 1e-06
MESH = pl.DeviceIdType.MESH
SIDE = 4
BLOCKS = 2 * SIDE
ORDER = (
    ("normalize", 0), ("prepare", 0), ("combine", 1), ("dispatch", 0), ("reduce", 1), ("finish", 1), ("experts", 0),
)
PIECES = 4
CAP = 6
F32 = jnp.float32
BF16 = jnp.bfloat16


def kernel(
    sizes,
    hidden_ref, routes_ref, probs_ref, gain_ref, wg_hbm, wu_hbm, wd_hbm,
    out_ref,
    wg, wu, wd, hs, grid, gmeta, outbox, inbox, back, part, parts, ysend, yrecv, acc,
    xin, sums, hid, turned, meta_t, pick, mix, shares, expect, perm,
    w_sem, ym_r, gm_r, gm_s, i_s, h_r, h_s, o_r, o_s,
    g_r, g_s, x_r, x_s, r_r, r_s, p_r, p_s, f_r, f_s,
):
    micro, tok, width, ff, local, stages = sizes
    half = width // 2
    span = half // PIECES
    order = [(c, h) for c in range(PIECES) for h in range(2)]
    rows = BLOCKS * CAP
    chunk = local * rows
    stage = lax.axis_index("pipe")
    e = lax.axis_index("exp")
    y = lax.axis_index("pair")
    x, z = e // SIDE, e % SIDE
    gather_at, send_at = (x, z), (z, x)

    def on_x(d):
        return {"exp": (x + d) % SIDE * SIDE + z}

    def on_z(d):
        return {"exp": x * SIDE + (z + d) % SIDE}

    gather_to, send_to = (on_x, on_z), (on_z, on_x)
    y_peer = {"pair": 1 - y}

    def push(src, dst, send, recv, to):
        pltpu.make_async_remote_copy(
            src_ref=src, dst_ref=dst, send_sem=send, recv_sem=recv, device_id=to, device_id_type=MESH
        ).start()

    def await_bytes(ref, sem):
        with jax.named_scope("wait"):
            pltpu.make_async_copy(ref, ref, sem).wait()

    weight_copies = [
        pltpu.make_async_copy(src.at[0], dst, w_sem.at[i])
        for i, (src, dst) in enumerate(((wg_hbm, wg), (wu_hbm, wu), (wd_hbm, wd)))
    ]
    for copy in weight_copies:
        copy.start()

    barrier = pltpu.get_barrier_semaphore()
    greeted = [y_peer] + [f(d) for f in (on_x, on_z) for d in range(1, SIDE)]
    greeted += [{"pipe": (stage + d) % stages} for d in (1, stages - 1)]
    greeted += [{"pipe": (stage + d) % stages, "pair": 1 - y} for d in (1, stages - 1)]
    for to in greeted:
        pl.semaphore_signal(barrier, inc=1, device_id=to, device_id_type=MESH)

    lane = lax.broadcasted_iota(jnp.int32, (tok, 128), 1)
    expert = (lane % 64).astype(F32)
    r0 = lax.broadcasted_iota(jnp.int32, (tok, tok), 0)
    r1 = lax.broadcasted_iota(jnp.int32, (tok, tok), 1)
    earlier = jnp.where(r1 < r0, 1.0, 0.0)
    eye = jnp.where(r1 == r0, 1.0, 0.0)
    last = (((1,), (1,)), ((), ()))
    for m in range(micro):
        chosen = lax.dot_general(eye, routes_ref[m].astype(F32), last, preferred_element_type=F32, precision="highest")
        probs = lax.dot_general(eye, probs_ref[m], last, preferred_element_type=F32, precision="highest")
        named = jnp.zeros((tok, 128), F32)
        weight = jnp.zeros((tok, 128), F32)
        for k in range(routes_ref.shape[1]):
            hit = chosen[:, k : k + 1] == expert
            named = jnp.where(hit, 1.0, named)
            weight = jnp.where(hit, probs[:, k : k + 1], weight)
        weight = weight / jnp.sum(probs, axis=-1, keepdims=True)
        before = jnp.dot(earlier, named, preferred_element_type=F32)
        both = jnp.where(lane < 64, named * (before + 1.0), weight).astype(BF16)
        for h in range(2):
            gmeta[h, gather_at[h] * 2 + y, m] = both

    q0 = lax.broadcasted_iota(jnp.int32, (rows, BLOCKS * tok), 0)
    q1 = lax.broadcasted_iota(jnp.int32, (rows, BLOCKS * tok), 1)
    expect[...] = jnp.where(q0 // CAP == q1 // tok, q0 % CAP + 1, -1).astype(F32)
    total = SIDE * rows
    piece = rows // SIDE
    s0 = lax.broadcasted_iota(jnp.int32, (total, total), 0)
    s1 = lax.broadcasted_iota(jnp.int32, (total, total), 1)
    perm[...] = jnp.where(
        s1 == s0 % rows // piece * rows + s0 // rows * piece + s0 % piece, 1.0, 0.0
    ).astype(BF16)

    @pl.when(stage == 0)
    def _():
        for m in range(micro):
            hs[m, y] = hidden_ref[m]

    with jax.named_scope("greet"):
        pl.semaphore_wait(barrier, len(greeted))

    def offer(m):
        push(hidden_ref.at[m], hs.at[m, y], i_s.at[m], o_r.at[m], y_peer)

    @pl.when(stage == 0)
    def _():
        offer(0)

    for h in range(2):
        tag = gmeta.at[h, gather_at[h] * 2 + y]
        push(tag, tag, gm_s.at[h], ym_r.at[h], y_peer)
        for d in (2, 1, 3):
            push(tag, tag, gm_s.at[h], gm_r.at[h], gather_to[h](d))

    with jax.named_scope("tags"):
        for h in range(2):
            tag = gmeta.at[h, gather_at[h] * 2 + 1 - y]
            await_bytes(tag, ym_r.at[h])
            for d in (2, 1, 3):
                push(tag, tag, gm_s.at[h], gm_r.at[h], gather_to[h](d))


    def prepare(m):
        for h in range(2):
            tags = gmeta[h, :, m].reshape(BLOCKS * tok, 128).astype(F32)
            meta_t[h] = tags.T
            for a in range(SIDE):
                owner = (x * SIDE + a) if h == 0 else (a * SIDE + z)
                for l in range(local):
                    at = (owner * 2 + y) * local + l
                    hit = meta_t[h, pl.ds(at, 1), :] == expect[...]
                    share = meta_t[h, pl.ds(64 + at, 1), :]
                    to = slice((a * local + l) * rows, (a * local + l + 1) * rows)
                    pick[h, to] = jnp.where(hit, 1.0, 0.0).astype(BF16)
                    mix[h, to] = jnp.where(hit, share, 0.0)
            shares[m % 2, h] = mix[h].T.astype(BF16)

    def normalize(m):
        @pl.when(stage > 0)
        def _():
            await_bytes(hs.at[m, y], h_r.at[m])

        for turn in range(2):
            pair = y if turn == 0 else 1 - y
            if turn == 1:
                await_bytes(hs.at[m, pair], o_r.at[m])
            floated = hs[m, pair].astype(F32)
            scale = lax.rsqrt(jnp.mean(floated * floated, axis=-1, keepdims=True) + EPS)
            normed = (floated * scale * gain_ref[...]).astype(BF16)
            for c, h in order:
                at = h * half + c * span
                grid[h, c, m, gather_at[h] * 2 + pair] = normed[:, at : at + span]
            for c, h in order:
                block = grid.at[h, c, m, gather_at[h] * 2 + pair]
                for d in (2, 1, 3):
                    push(block, block, g_s.at[h, c, m], g_r.at[h, c, m], gather_to[h](d))

    def dispatch(m):
        for c, h in order:
            await_bytes(grid.at[h, c, m, 0 : BLOCKS - 2], g_r.at[h, c, m])
            chosen = jnp.dot(
                pick[h], grid[h, c, m].reshape(BLOCKS * tok, span), preferred_element_type=F32
            ).astype(BF16)
            outbox[h, c, m] = chosen.reshape(SIDE, local, rows, span)
            own = send_at[h]
            for d in (2, 1, 3):
                push(
                    outbox.at[h, c, m, (own + d) % SIDE], inbox.at[h, c, m, own],
                    x_s.at[h, c, m], x_r.at[h, c, m], send_to[h](d),
                )
            inbox[h, c, m, own] = outbox[h, c, m, own]

    def experts(m):
        for c in range(PIECES):
            for h in range(2):
                await_bytes(inbox.at[h, c, m, 0 : SIDE - 1], x_r.at[h, c, m])
                await_bytes(outbox.at[h, c, m, 0 : SIDE - 1], x_s.at[h, c, m])
            for l in range(local):
                xin[l] = jnp.dot(
                    perm[...], inbox[1, c, m, :, l].reshape(total, span), preferred_element_type=F32
                ).astype(BF16)
            low, high = slice(c * span, (c + 1) * span), slice(half + c * span, half + (c + 1) * span)
            for l in range(local):
                for n in range(0, ff, 256):
                    to = slice(n, n + 256)
                    gate, upward = [
                        jnp.dot(inbox[0, c, m, :, l].reshape(total, span), w[l, low, to], preferred_element_type=F32)
                        + jnp.dot(xin[l], w[l, high, to], preferred_element_type=F32)
                        for w in (wg, wu)
                    ]
                    if c > 0:
                        gate, upward = gate + sums[0, l, :, to], upward + sums[1, l, :, to]
                    if c < PIECES - 1:
                        sums[0, l, :, to], sums[1, l, :, to] = gate, upward
                    else:
                        hid[l, :, to] = (jax.nn.silu(gate) * upward).astype(BF16)
        for c, h in order:
            for l in range(local):
                if h == 1 and c == 0:
                    turned[l] = jnp.dot(perm[...], hid[l], preferred_element_type=F32).astype(BF16)
                for n in range(0, span, 256):
                    at = h * half + c * span + n
                    made = jnp.dot(
                        hid[l] if h == 0 else turned[l], wd[l, :, at : at + 256], preferred_element_type=F32
                    )
                    outbox[h, c, m, :, l, :, n : n + 256] = made.astype(BF16).reshape(SIDE, rows, 256)
            own = send_at[h]
            for d in (2, 1, 3):
                push(
                    outbox.at[h, c, m, (own + d) % SIDE], back.at[h, c, m, own],
                    r_s.at[h, c, m], r_r.at[h, c, m], send_to[h](d),
                )
            back[h, c, m, own] = outbox[h, c, m, own]

    def combine(m):
        for c, h in order:
            await_bytes(back.at[h, c, m, 0 : SIDE - 1], r_r.at[h, c, m])
            summed = jnp.dot(
                shares[m % 2, h], back[h, c, m].reshape(SIDE * chunk, span), preferred_element_type=F32
            )
            part[h, c, m] = summed.astype(BF16).reshape(SIDE, 2 * tok, span)
            own = gather_at[h]
            for d in (2, 1, 3):
                push(
                    part.at[h, c, m, (own + d) % SIDE], parts.at[h, c, m, own],
                    p_s.at[h, c, m], p_r.at[h, c, m], gather_to[h](d),
                )

    def reduce(m):
        for c, h in order:
            await_bytes(parts.at[h, c, m, 0 : SIDE - 1], p_r.at[h, c, m])
            own = gather_at[h]

            def total_of(side):
                at = pl.ds(pl.multiple_of(side * tok, tok), tok)
                value = part[h, c, m, own, at].astype(F32)
                for d in range(1, SIDE):
                    value = value + parts[h, c, m, (own + d) % SIDE, at].astype(F32)
                return value

            ysend[h, c, m] = total_of(1 - y).astype(BF16)
            push(ysend.at[h, c, m], yrecv.at[h, c, m], f_s.at[h, c, m], f_r.at[h, c, m], y_peer)
            acc[h, c] = total_of(y)

    def finish(m):
        for c, h in order:
            await_bytes(yrecv.at[h, c, m], f_r.at[h, c, m])
            at = slice(h * half + c * span, h * half + (c + 1) * span)
            out_ref[m, :, at] = (
                hs[m, y, :, at].astype(F32) + (acc[h, c] + yrecv[h, c, m].astype(F32))
            ).astype(BF16)

            @pl.when(stage < stages - 1)
            def _():
                done, there = out_ref.at[m, :, at], hs.at[m, y, :, at]
                push(done, there, o_s.at[m], o_r.at[m], {"pipe": stage + 1, "pair": 1 - y})
                push(done, there, h_s.at[m], h_r.at[m], {"pipe": stage + 1})

    tasks = {
        "prepare": prepare, "normalize": normalize, "dispatch": dispatch, "experts": experts,
        "combine": combine, "reduce": reduce, "finish": finish,
    }

    def step(i, _):
        for name, lag in ORDER:

            @pl.when((i >= lag) & (i < micro + lag))
            def _():
                with jax.named_scope(name):
                    if name == "experts":

                        @pl.when(i == lag)
                        def _():
                            for copy in weight_copies:
                                copy.wait()

                    if name == "prepare":

                        @pl.when(i == lag)
                        def _():
                            for h in range(2):
                                await_bytes(gmeta.at[h, 0 : BLOCKS - 2], gm_r.at[h])

                        @pl.when((i == lag) & (stage == 0))
                        def _():
                            for m in range(1, micro):
                                offer(m)

                    tasks[name](i - lag)

        return 0

    lax.fori_loop(0, micro + max(lag for _, lag in ORDER), step, 0)

    for h in range(2):
        await_bytes(gmeta.at[h, 0 : BLOCKS - 1], gm_s.at[h])

    def drain(m, _):
        for c, h in order:
            await_bytes(grid.at[h, c, m, 0 : BLOCKS - 2], g_s.at[h, c, m])
            await_bytes(outbox.at[h, c, m, 0 : SIDE - 1], r_s.at[h, c, m])
            await_bytes(part.at[h, c, m, 0 : SIDE - 1], p_s.at[h, c, m])
            await_bytes(ysend.at[h, c, m], f_s.at[h, c, m])

        @pl.when(stage == 0)
        def _():
            await_bytes(hidden_ref.at[m], i_s.at[m])

        @pl.when(stage < stages - 1)
        def _():
            await_bytes(out_ref.at[m], h_s.at[m])
            await_bytes(out_ref.at[m], o_s.at[m])

        return 0

    lax.fori_loop(0, micro, drain, 0)


def on_device(stages, hidden_in, routes, gate_probs, norm_gain, w_gate, w_up, w_down):
    micro, tok, width = hidden_in.shape
    local, ff = w_gate.shape[1], w_gate.shape[3]
    span = width // 2 // PIECES
    rows = BLOCKS * CAP
    sizes = (micro, tok, width, ff, local, stages)
    vmem = pl.BlockSpec(memory_space=pltpu.VMEM)
    hbm = pl.BlockSpec(memory_space=pl.ANY)
    pair = pltpu.SemaphoreType.DMA((2, PIECES, micro))
    halves = pltpu.SemaphoreType.DMA((2,))
    single = pltpu.SemaphoreType.DMA((micro,))
    out = pl.pallas_call(
        functools.partial(kernel, sizes),
        out_shape=jax.ShapeDtypeStruct((micro, tok, width), BF16),
        in_specs=[vmem, vmem, vmem, vmem, hbm, hbm, hbm],
        out_specs=vmem,
        scratch_shapes=[
            pltpu.VMEM((local, width, ff), BF16),
            pltpu.VMEM((local, width, ff), BF16),
            pltpu.VMEM((local, ff, width), BF16),
            pltpu.VMEM((micro, 2, tok, width), BF16),
            pltpu.VMEM((2, PIECES, micro, BLOCKS, tok, span), BF16),
            pltpu.VMEM((2, BLOCKS, micro, tok, 128), BF16),
            pltpu.VMEM((2, PIECES, micro, SIDE, local, rows, span), BF16),
            pltpu.VMEM((2, PIECES, micro, SIDE, local, rows, span), BF16),
            pltpu.VMEM((2, PIECES, micro, SIDE, local, rows, span), BF16),
            pltpu.VMEM((2, PIECES, micro, SIDE, 2 * tok, span), BF16),
            pltpu.VMEM((2, PIECES, micro, SIDE, 2 * tok, span), BF16),
            pltpu.VMEM((2, PIECES, micro, tok, span), BF16),
            pltpu.VMEM((2, PIECES, micro, tok, span), BF16),
            pltpu.VMEM((2, PIECES, tok, span), F32),
            pltpu.VMEM((local, SIDE * rows, span), BF16),
            pltpu.VMEM((2, local, SIDE * rows, ff), F32),
            pltpu.VMEM((local, SIDE * rows, ff), BF16),
            pltpu.VMEM((local, SIDE * rows, ff), BF16),
            pltpu.VMEM((2, 128, BLOCKS * tok), F32),
            pltpu.VMEM((2, SIDE * local * rows, BLOCKS * tok), BF16),
            pltpu.VMEM((2, SIDE * local * rows, BLOCKS * tok), F32),
            pltpu.VMEM((2, 2, BLOCKS * tok, SIDE * local * rows), BF16),
            pltpu.VMEM((rows, BLOCKS * tok), F32),
            pltpu.VMEM((SIDE * rows, SIDE * rows), BF16),
            pltpu.SemaphoreType.DMA((3,)),
            halves, halves, halves, single, single, single, single, single,
            pair, pair, pair, pair, pair, pair, pair, pair, pair, pair,
        ],
        compiler_params=pltpu.CompilerParams(
            collective_id=0, has_side_effects=True, vmem_limit_bytes=67043328
        ),
        name="relay",
    )(
        hidden_in,
        jnp.swapaxes(routes[0], 1, 2),
        jnp.swapaxes(gate_probs[0], 1, 2),
        norm_gain,
        w_gate,
        w_up,
        w_down,
    )
    return out[None]


def solution(mesh):
    in_specs = (
        P(None, ("exp", "pair"), None),
        P("pipe", None, ("exp", "pair"), None),
        P("pipe", None, ("exp", "pair"), None),
        P("pipe", None),
        P("pipe", ("exp", "pair"), None, None),
        P("pipe", ("exp", "pair"), None, None),
        P("pipe", ("exp", "pair"), None, None),
    )
    out_specs = P("pipe", None, ("exp", "pair"), None)
    return jax.shard_map(
        functools.partial(on_device, mesh.shape["pipe"]),
        mesh=mesh,
        in_specs=in_specs,
        out_specs=out_specs,
        check_vma=False,
    )
```
